32 devices in a mesh: shard: 2 (over core), ctx: 4 (over y, x), tp: 4 (over z).
Axes of the slice: x: 2, y: 2, z: 4, core: 2. Of those that a mesh axis runs over, the one named last changes fastest.
Arguments:
- tokens: bfloat16 [2, 4096, 1024], P('shard', 'ctx'), may hold values from -6 to 6
- lengths: int32 [2], P('shard'), may hold values from 1024 to 4096, as said below
- routes: int32 [2, 4096, 1], P('shard', 'ctx'), may hold values from 0 to 7; in each aligned block of 1024 rows (0 to 1023, 1024 to 2047, ..., all dimensions but the last counted through in order) at most 384 rows name the same one
- priority: int32 [2, 4096], P('shard', 'ctx'), may hold values from 0 to 8191, as said below
- attn_gain: bfloat16 [1024], P(('shard', 'ctx')), may hold values from 0.5 to 1.5
- qkv_weight: bfloat16 [1024, 3, 1024], P(('shard', 'ctx'), None, 'tp'), may hold values from -0.1875 to 0.1875
- proj_weight: bfloat16 [1024, 1024], P('tp', ('shard', 'ctx')), may hold values from -2 to 2
- ffn_gain: bfloat16 [1024], P(('shard', 'ctx')), may hold values from 0.5 to 1.5
- mix_weight: bfloat16 [1024, 2], P(('shard', 'ctx')), may hold values from -0.1875 to 0.1875
- up_weight: bfloat16 [1024, 4096], P(('shard', 'ctx'), 'tp'), may hold values from -0.1875 to 0.1875
- down_weight: bfloat16 [4096, 1024], P('tp', ('shard', 'ctx')), may hold values from -0.09375 to 0.09375
- expert_up: bfloat16 [8, 1024, 4096], P(('shard', 'ctx'), None, 'tp'), may hold values from -0.1875 to 0.1875
- expert_down: bfloat16 [8, 4096, 1024], P(('shard', 'ctx'), 'tp'), may hold values from -0.09375 to 0.09375
- cotangent: bfloat16 [2, 4096, 1024], P('shard', 'ctx'), may hold values from -6 to 6
Outputs:
- layer_out: bfloat16 [2, 4096, 1024], P('shard', 'ctx')
- tokens_grad: bfloat16 [2, 4096, 1024], P('shard', 'ctx')
- attn_gain_grad: float32 [1024], P(('shard', 'ctx'))
- qkv_weight_grad: float32 [1024, 3, 1024], P(('shard', 'ctx'), None, 'tp')
- proj_weight_grad: float32 [1024, 1024], P('tp', ('shard', 'ctx'))
- ffn_gain_grad: float32 [1024], P(('shard', 'ctx'))
- mix_weight_grad: float32 [1024, 2], P(('shard', 'ctx'))
- up_weight_grad: float32 [1024, 4096], P(('shard', 'ctx'), 'tp')
- down_weight_grad: float32 [4096, 1024], P('tp', ('shard', 'ctx'))
- expert_up_grad: float32 [8, 1024, 4096], P(('shard', 'ctx'), None, 'tp')
- expert_down_grad: float32 [8, 4096, 1024], P(('shard', 'ctx'), 'tp')
The draws below stay inside these ranges and needn't reach their ends.
Inputs may be any that keep to these rules, and one draw needn't show every extreme that they name: `lengths`: padding positions are those at or past a slot's length; some slot has exactly 4096 live positions. `routes`: in the rows of one device (one slot's 1024 positions on one index of ctx), at most 384 positions name the same expert, and exactly 384 do for some expert on some device. `priority`: each value 0 to 8191 occurs at exactly one position of all slots.
All inputs are finite; a program needn't handle non-finite values.
Results may differ from the reference program's by a relative error of at most 0.024.
Values may be sent and summed in bfloat16 or wider, within the bound.
A program may use at most 192 MiB of HBM per device.

```python
import math
import jax
import jax.numpy as jnp
import numpy as np
from jax import lax

D = 1024
HEADS = 16
HD = 64
FF = 4096
SEQ_DEV = 1024
SEQ = 4096
SLOTS = 2
EXPERTS = 8
SLOT_CAP = 384
CAP = 1152


def draw_lengths(key, part):
    first_key, second_key = jax.random.split(key)
    drawn = jax.random.randint(first_key, (SLOTS,), SEQ // 4, SEQ + 1)
    longest = jax.random.randint(second_key, (), 0, SLOTS)
    return drawn.at[longest].set(SEQ).astype(jnp.int32)


def draw_priority(key, part):
    return jax.random.permutation(key, SLOTS * SEQ).astype(jnp.int32).reshape(SLOTS, SEQ)


def spiked(values, rng, source, target, parts, factor):
    owner, partner = [(jnp.arange(values.shape[axis_at]) // (values.shape[axis_at] // parts)).reshape([-1 if axis == axis_at else 1 for axis in range(values.ndim)]) for axis_at in (source, target)]
    chosen = jax.random.permutation(rng, parts)[partner]
    strong = (owner == chosen) | (owner == (partner + parts // 2) % parts)
    return jnp.where(strong, factor * values, values)


def steps_of(stream_key, dims, cuts, smallest, top_value):
    def one(position, parts):
        draws = jax.random.uniform(jax.random.fold_in(jax.random.fold_in(stream_key, 6), position), (parts,), jnp.float32, smallest / len(cuts), top_value / len(cuts))
        return jnp.repeat(jnp.exp(draws), dims[position] // parts).reshape((-1,) + (1,) * (len(dims) - position - 1))

    factor_of = one(*cuts[0])
    for cut in cuts[1:]:
        factor_of = factor_of * one(*cut)
    return factor_of


def assign_block(stream_key, own, number, rows, count, top, limit, slope):
    order = jax.random.permutation(stream_key, count)
    heavy_load, usual = portions_of(count, rows * top, limit, slope, True), portions_of(count, rows * top, limit, slope, False)
    places = jnp.arange(count)

    def named(tallies, turn):
        used = int((tallies > 0).sum())
        fixed = max(1, used // 4)
        passed = fixed + (places - fixed + turn * (used - fixed)) % max(1, count - fixed)
        return jnp.zeros((count,), jnp.int32).at[order[jnp.where(places < fixed, places, passed)]].set(jnp.asarray(tallies, jnp.int32))

    tallies = jnp.where(number % 4 == 0, named(heavy_load, number // 4), named(usual, number - number // 4 - 1))
    mixed = jax.random.permutation(jax.random.fold_in(own, 3), count)
    source_of, receiver = mixed[0:count // 2 * 2:2], mixed[1:count // 2 * 2:2]
    margin = jnp.minimum(tallies[source_of] - 1, limit - tallies[receiver]) // 2
    margin = jnp.where((source_of == order[0]) | (receiver == order[0]) | (tallies[receiver] == 0), 0, jnp.maximum(margin, 0))
    passed = jax.random.randint(jax.random.fold_in(own, 4), (count // 2,), 0, 1 << 20) % (margin + 1)
    tallies = tallies.at[source_of].add(-passed).at[receiver].add(passed)
    items = jnp.searchsorted(jnp.cumsum(tallies), jnp.arange(rows * top), side="right").astype(jnp.int32)
    grid = items.reshape(top, rows).T
    grid = grid[jax.random.permutation(jax.random.fold_in(own, 1), rows)]
    turn = jax.random.randint(jax.random.fold_in(own, 2), (rows, 1), 0, top)
    return jnp.take_along_axis(grid, (jnp.arange(top)[None, :] + turn) % top, axis=1)


def portions_of(number_of, total, reach, slope, full):
    loads = [(1 << 20) // math.isqrt(grade ** slope) + 1 for grade in range(1, number_of + 1)]
    largest = reach if full else min(reach, max(-(-total // number_of), total * loads[0] // sum(loads)))
    least = 1 if total - largest >= number_of - 1 else 0
    holding, rest = [largest] + [least] * (number_of - 1), total - largest - least * (number_of - 1)
    while rest > 0:
        movable = [i for i in range(1, number_of) if holding[i] < largest] or [i for i in range(1, number_of) if holding[i] < reach]
        mass, left = sum([loads[i] for i in movable]), rest
        for i in movable:
            addition = min(reach - holding[i], max(1, left * loads[i] // mass), rest)
            holding[i] = holding[i] + addition
            rest = rest - addition
    return np.array(holding)


def bell_draw(stream_key, extent, width, bound, shards=(), held_as=jnp.bfloat16):
    values = jax.random.normal(stream_key, extent, jnp.float32) * width
    if len(shards) > 0:
        values = steps_of(stream_key, extent, shards, -0.22, 0.18) * values
    return jnp.clip(values, min=-bound, max=bound).astype(held_as)


def noise_with(rng, extent, deviation, most, cuts, heavy, kind=jnp.bfloat16):
    array = deviation * jax.random.normal(rng, extent, jnp.float32)
    if cuts:
        array = array * steps_of(rng, extent, cuts, -0.22, 0.18)
    return jnp.clip(spiked(array, jax.random.fold_in(rng, 3), *heavy), -most, most).astype(kind)


def setup_inputs(seed: int = 0) -> dict:
    streams_of = jax.random.split(jax.random.key(seed), 15)
    tokens = bell_draw(streams_of[0], (SLOTS, SEQ, D), 1.0, 6.0, ((0, 2), (1, 4)))
    lengths = draw_lengths(jax.random.fold_in(streams_of[14], 71), 0)
    routes_keys = jax.random.split(jax.random.fold_in(streams_of[2], 1), SLOTS * SEQ // SEQ_DEV)
    routes_turns = jax.random.permutation(jax.random.fold_in(streams_of[2], 3), SLOTS * SEQ // SEQ_DEV)
    routes = jax.vmap(lambda own, number: assign_block(jax.random.fold_in(streams_of[2], 2), own, number, SEQ_DEV, EXPERTS, 1, SLOT_CAP, 2))(routes_keys, routes_turns).reshape((SLOTS, SEQ, 1))
    priority = draw_priority(jax.random.fold_in(streams_of[14], 71), 0)
    attn_gain = jnp.clip(1.0 + 0.1 * jax.random.normal(streams_of[4], (D,), jnp.float32), 0.5, 1.5).astype(jnp.bfloat16)
    qkv_weight = bell_draw(streams_of[5], (D, 3, D), D ** -0.5, 0.1875, ((0, 8), (2, 4)))
    proj_weight = bell_draw(streams_of[6], (D, D), (max(1, D // 128)) ** -0.5, 2.0, ((0, 4), (1, 8)))
    ffn_gain = jnp.clip(1.0 + 0.1 * jax.random.normal(streams_of[7], (D,), jnp.float32), 0.5, 1.5).astype(jnp.bfloat16)
    mix_weight = bell_draw(streams_of[8], (D, 2), D ** -0.5, 0.1875, ((0, 8),))
    up_weight = bell_draw(streams_of[9], (D, FF), D ** -0.5, 0.1875, ((0, 8), (1, 4)))
    down_weight = bell_draw(streams_of[10], (FF, D), FF ** -0.5, 0.09375, ((0, 4), (1, 8)))
    expert_up = bell_draw(streams_of[11], (EXPERTS, D, FF), D ** -0.5, 0.1875, ((0, 8), (2, 4)))
    expert_down = bell_draw(streams_of[12], (EXPERTS, FF, D), FF ** -0.5, 0.09375, ((0, 8), (1, 4)))
    cotangent = noise_with(streams_of[13], (SLOTS, SEQ, D), 1.0, 6.0, ((0, 2), (1, 4)), (0, 2, 2, 2.0))
    return dict(tokens=tokens, lengths=lengths, routes=routes, priority=priority, attn_gain=attn_gain, qkv_weight=qkv_weight, proj_weight=proj_weight, ffn_gain=ffn_gain, mix_weight=mix_weight, up_weight=up_weight, down_weight=down_weight, expert_up=expert_up, expert_down=expert_down, cotangent=cotangent)


@jax.custom_vjp
def low(v):
    return lax.optimization_barrier(v.astype(jnp.bfloat16)).astype(jnp.float32)

@jax.custom_vjp
def low_back(v):
    return v

def low_keep(v):
    return (low(v), None)

def low_pass(kept, grad):
    return (grad,)

def back_keep(v):
    return (v, None)

def back_low(kept, grad):
    return (low(grad),)
low.defvjp(low_keep, low_pass)
low_back.defvjp(back_keep, back_low)

def layer_norm(values, gain_vec):
    average = lax.optimization_barrier(jnp.mean(values, axis=-1, keepdims=True))
    centred = values - average
    spread = lax.optimization_barrier(jnp.mean(centred * centred, axis=-1, keepdims=True))
    return centred * lax.rsqrt(spread + 1e-05) * gain_vec

def product(form, left, right):
    return jnp.einsum(form, left, right, precision=lax.Precision.HIGHEST)

def gelu_tanh(values):
    return jax.nn.gelu(values, approximate=True)

def attend_slot(inputs):
    queries, key_rows, value_rows, length = inputs
    qblock = min(512, SEQ)
    positions = jnp.arange(SEQ, dtype=jnp.int32)
    key_live = positions < length
    score_scale = HD ** (-0.5)

    def one_block(row_start):
        row_block = lax.dynamic_slice_in_dim(queries, row_start, qblock, 0)
        scores = low_back(product('qhd,khd->hqk', row_block, key_rows) * score_scale)
        rowpos = row_start + jnp.arange(qblock, dtype=jnp.int32)
        allowed = (positions[None, :] <= rowpos[:, None]) & key_live[None, :]
        scores = jnp.where(allowed[None], scores, -1e+30)
        weights = low(jax.nn.softmax(scores, axis=-1))
        return product('hqk,khd->qhd', weights, value_rows)
    starts = jnp.arange(0, SEQ, qblock, dtype=jnp.int32)
    blocks = lax.map(jax.checkpoint(one_block), starts)
    return blocks.reshape(SEQ, HEADS, HD)

def route_tables(routes, priority, lengths):
    token_count = SLOTS * SEQ
    chosen = routes[..., 0].reshape(token_count).astype(jnp.int32)
    order_key = priority.reshape(token_count).astype(jnp.int32)
    live_mask = (jnp.arange(SEQ, dtype=jnp.int32)[None, :] < lengths[:, None]).reshape(token_count)
    sort_key = jnp.where(live_mask, chosen * token_count + order_key, EXPERTS * token_count + order_key)
    sorted_order = jnp.argsort(sort_key).astype(jnp.int32)
    sort_place = jnp.zeros((token_count,), jnp.int32).at[sorted_order].set(jnp.arange(token_count, dtype=jnp.int32))
    member = (chosen[None, :] == jnp.arange(EXPERTS, dtype=jnp.int32)[:, None]) & live_mask[None, :]
    expert_loads = lax.optimization_barrier(jnp.sum(member.astype(jnp.int32), axis=1)).astype(jnp.int32)
    expert_starts = (jnp.cumsum(expert_loads) - expert_loads).astype(jnp.int32)
    queue_rank = (sort_place - expert_starts[chosen]).astype(jnp.int32)
    kept_mask = live_mask & (queue_rank < CAP)
    target = jnp.where(kept_mask, chosen * CAP + queue_rank, EXPERTS * CAP).astype(jnp.int32)
    take_index = jnp.zeros((EXPERTS * CAP,), jnp.int32).at[target].set(jnp.arange(token_count, dtype=jnp.int32), mode='drop')
    take_valid = jnp.zeros((EXPERTS * CAP,), jnp.float32).at[target].set(1.0, mode='drop')
    token_slot = jnp.where(kept_mask, chosen * CAP + queue_rank, 0).astype(jnp.int32)
    return (take_index, take_valid, token_slot, kept_mask.astype(jnp.float32), live_mask.astype(jnp.float32))

def forward(tokens, attn_gain, qkv_weight, proj_weight, ffn_gain, mix_weight, up_weight, down_weight, expert_up, expert_down, tables):
    take_index, take_valid, token_slot, kept_mask, live_mask, lengths = tables
    live_rows = live_mask.reshape(SLOTS, SEQ, 1)
    normed = low(layer_norm(tokens, attn_gain))
    projected = low(low_back(product('std,dcf->stcf', normed, qkv_weight)))
    queries = projected[:, :, 0].reshape(SLOTS, SEQ, HEADS, HD)
    key_rows = projected[:, :, 1].reshape(SLOTS, SEQ, HEADS, HD)
    value_rows = projected[:, :, 2].reshape(SLOTS, SEQ, HEADS, HD)
    attended = lax.map(attend_slot, (queries, key_rows, value_rows, lengths))
    attended = low(low_back(attended.reshape(SLOTS, SEQ, D)))
    branch = low_back(product('stf,fd->std', attended, proj_weight))
    middle = tokens + branch
    normed2 = low(layer_norm(middle, ffn_gain))
    mixing = jax.nn.softmax(product('std,dk->stk', normed2, mix_weight), axis=-1)
    upper_pre = low_back(product('std,df->stf', normed2, up_weight))
    hidden = low(gelu_tanh(upper_pre))
    dense_out = low_back(product('stf,fd->std', hidden, down_weight))
    flat_rows = normed2.reshape(SLOTS * SEQ, D)
    gathered = (flat_rows[take_index] * take_valid[:, None]).reshape(EXPERTS, CAP, D)
    expert_pre = low_back(product('ecd,edf->ecf', gathered, expert_up))
    expert_hidden = low(gelu_tanh(expert_pre))
    expert_rows = product('ecf,efd->ecd', expert_hidden, expert_down).reshape(EXPERTS * CAP, D)
    expert = low_back((expert_rows[token_slot] * kept_mask[:, None]).reshape(SLOTS, SEQ, D))
    result = middle + mixing[..., 0:1] * dense_out + mixing[..., 1:2] * expert
    return result * live_rows

def reference(tokens, lengths, routes, priority, attn_gain, qkv_weight, proj_weight, ffn_gain, mix_weight, up_weight, down_weight, expert_up, expert_down, cotangent):
    take_index, take_valid, token_slot, kept_mask, live_mask = route_tables(routes, priority, lengths)
    tables = (take_index, take_valid, token_slot, kept_mask, live_mask, lengths.astype(jnp.int32))
    primals = (tokens, attn_gain, qkv_weight, proj_weight, ffn_gain, mix_weight, up_weight, down_weight, expert_up, expert_down)
    primals = [value.astype(jnp.float32) for value in primals]

    def apply_layer(*values):
        return forward(*values, tables)
    result, pullback = jax.vjp(apply_layer, *primals)
    gradients = pullback(cotangent.astype(jnp.float32))
    return (result.astype(jnp.bfloat16), gradients[0].astype(jnp.bfloat16), gradients[1], gradients[2], gradients[3], gradients[4], gradients[5], gradients[6], gradients[7], gradients[8], gradients[9])
```

```python
import jax
import jax.numpy as jnp
from jax import lax
from jax.experimental import pallas as pl
from jax.experimental.pallas import tpu as pltpu
from jax.sharding import PartitionSpec as P

HD = 64
CAP = 1152
TILE = 512


empty_mark = 1 << 30
norm_eps = 1e-05
masked_score = -1e30


def gelu_tanh(values):
    return jax.nn.gelu(values, approximate=True)


def norm_forward(values, gain_vec):
    average = jnp.mean(values, axis=-1, keepdims=True)
    centred = values - average
    spread = jnp.mean(centred * centred, axis=-1, keepdims=True)
    inverse = lax.rsqrt(spread + norm_eps)
    unit_rows = centred * inverse
    return (unit_rows * gain_vec, unit_rows, inverse)


def norm_backward(upstream, gain_vec, unit_rows, inverse):
    shaped = upstream * gain_vec
    first_term = jnp.mean(shaped, axis=-1, keepdims=True)
    second_term = jnp.mean(shaped * unit_rows, axis=-1, keepdims=True)
    return (
        inverse * (shaped - first_term - unit_rows * second_term),
        jnp.sum(upstream * unit_rows, axis=0),
    )

NT = (((1,), (1,)), ((), ()))


def tile_of(index, chunk):
    per = chunk // TILE
    return index // per, pl.ds(pl.multiple_of((index % per) * TILE, TILE), TILE)


def rows_of(index):
    return pl.ds(pl.multiple_of(index * TILE, TILE), TILE)


def causal():
    key_at = lax.broadcasted_iota(jnp.int32, (TILE, TILE), 0)
    query_at = lax.broadcasted_iota(jnp.int32, (TILE, TILE), 1)
    return key_at <= query_at


def flash_forward_body(qkv_ref, out_ref, wide_ref, lse_ref, key_rows):
    chunks, _, _, chunk = qkv_ref.shape
    tiles = chunks * chunk // TILE
    for c in range(chunks):
        key_rows[pl.ds(c * chunk, chunk), :] = qkv_ref[c, 1].T

    @pl.loop(0, tiles)
    def _(i):
        c, at = tile_of(i, chunk)
        query = qkv_ref[c, 0, :, at] * (HD ** (-0.5))

        def step(j, state, mask):
            top, total, acc = state
            kc, kat = tile_of(j, chunk)
            scores = jnp.dot(key_rows[rows_of(j), :], query, preferred_element_type=jnp.float32)
            if mask:
                scores = jnp.where(causal(), scores, masked_score)
            new_top = jnp.maximum(top, jnp.max(scores, axis=0, keepdims=True))
            shrink = jnp.exp(top - new_top)
            weights = jnp.exp(scores - new_top)
            total = total * shrink + jnp.sum(weights, axis=0, keepdims=True)
            acc = acc * shrink + jnp.dot(
                qkv_ref[kc, 2, :, kat],
                weights.astype(jnp.bfloat16),
                preferred_element_type=jnp.float32,
            )
            return new_top, total, acc

        state = (
            jnp.full((1, TILE), masked_score, jnp.float32),
            jnp.zeros((1, TILE), jnp.float32),
            jnp.zeros((HD, TILE), jnp.float32),
        )
        state = step(i, state, True)
        top, total, acc = lax.fori_loop(0, i, lambda j, s: step(j, s, False), state)
        result = acc / total
        wide_ref[c, :, at] = result
        out_ref[c, :, at] = result.astype(jnp.bfloat16)
        lse_ref[c, :, at] = top + jnp.log(total)


def flash_forward(qkv):
    chunks, _, width, chunk = qkv.shape
    return pl.pallas_call(
        flash_forward_body,
        name="flash_forward",
        out_shape=(
            jax.ShapeDtypeStruct((chunks, width, chunk), jnp.bfloat16),
            jax.ShapeDtypeStruct((chunks, width, chunk), jnp.float32),
            jax.ShapeDtypeStruct((chunks, 1, chunk), jnp.float32),
        ),
        scratch_shapes=[pltpu.VMEM((chunks * chunk, width), jnp.bfloat16)],
        cost_estimate=pl.CostEstimate(
            flops=2 * (chunks * chunk) ** 2 * width * 4, bytes_accessed=5 << 20, transcendentals=0
        ),
        compiler_params=pltpu.CompilerParams(vmem_limit_bytes=40 << 20),
    )(qkv)


def flash_backward_body(
    qkv_ref, grad_ref, wide_ref, lse_ref, out_ref,
    query_cols, query_rows, key_rows, value_rows, grad_rows, delta, query_grad,
):
    chunks, _, _, chunk = qkv_ref.shape
    tiles = chunks * chunk // TILE
    scale = HD ** (-0.5)
    for c in range(chunks):
        at = pl.ds(c * chunk, chunk)
        scaled = qkv_ref[c, 0] * scale
        query_cols[c] = scaled
        query_rows[at, :] = scaled.T
        key_rows[at, :] = qkv_ref[c, 1].T
        value_rows[at, :] = qkv_ref[c, 2].T
        grad_rows[at, :] = grad_ref[c].T
        delta[c] = jnp.sum(
            grad_ref[c].astype(jnp.float32) * wide_ref[c], axis=0, keepdims=True
        )
        query_grad[c] = jnp.zeros((HD, chunk), jnp.float32)

    @pl.loop(0, tiles)
    def _(j):
        kc, kat = tile_of(j, chunk)
        key_tile = key_rows[rows_of(j), :]
        value_tile = value_rows[rows_of(j), :]
        key_cols = qkv_ref[kc, 1, :, kat]

        def step(i, state, mask):
            key_grad, value_grad = state
            c, at = tile_of(i, chunk)
            scores = jnp.dot(key_tile, query_cols[c, :, at], preferred_element_type=jnp.float32)
            probs = jnp.exp(scores - lse_ref[c, :, at])
            if mask:
                probs = jnp.where(causal(), probs, 0.0)
            prob_grad = jnp.dot(value_tile, grad_ref[c, :, at], preferred_element_type=jnp.float32)
            score_grad = (probs * (prob_grad - delta[c, :, at])).astype(jnp.bfloat16)
            value_grad += jnp.dot(
                probs.astype(jnp.bfloat16), grad_rows[rows_of(i), :],
                preferred_element_type=jnp.float32,
            )
            key_grad += jnp.dot(
                score_grad, query_rows[rows_of(i), :], preferred_element_type=jnp.float32
            )
            query_grad[c, :, at] += jnp.dot(
                key_cols, score_grad, preferred_element_type=jnp.float32
            )
            return key_grad, value_grad

        state = (jnp.zeros((TILE, HD), jnp.float32), jnp.zeros((TILE, HD), jnp.float32))
        state = step(j, state, True)
        key_grad, value_grad = lax.fori_loop(
            j + 1, tiles, lambda i, s: step(i, s, False), state
        )
        out_ref[kc, 1, :, kat] = key_grad.T.astype(jnp.bfloat16)
        out_ref[kc, 2, :, kat] = value_grad.T.astype(jnp.bfloat16)

    for c in range(chunks):
        out_ref[c, 0] = (query_grad[c] * scale).astype(jnp.bfloat16)


def flash_backward(qkv, grad, wide, lse):
    chunks, _, width, chunk = qkv.shape
    full = chunks * chunk
    return pl.pallas_call(
        flash_backward_body,
        name="flash_backward",
        out_shape=jax.ShapeDtypeStruct((chunks, 3, width, chunk), jnp.bfloat16),
        scratch_shapes=[
            pltpu.VMEM((chunks, width, chunk), jnp.bfloat16),
            pltpu.VMEM((full, width), jnp.bfloat16),
            pltpu.VMEM((full, width), jnp.bfloat16),
            pltpu.VMEM((full, width), jnp.bfloat16),
            pltpu.VMEM((full, width), jnp.bfloat16),
            pltpu.VMEM((chunks, 1, chunk), jnp.float32),
            pltpu.VMEM((chunks, width, chunk), jnp.float32),
        ],
        cost_estimate=pl.CostEstimate(
            flops=2 * full ** 2 * width * 10, bytes_accessed=8 << 20, transcendentals=0
        ),
        compiler_params=pltpu.CompilerParams(vmem_limit_bytes=48 << 20),
    )(qkv, grad, wide, lse)


def local(
    tokens,
    lengths,
    routes,
    priority,
    attn_gain,
    qkv_weight,
    proj_weight,
    ffn_gain,
    mix_weight,
    up_weight,
    down_weight,
    expert_up,
    expert_down,
    cotangent,
):
    seq_dev = tokens.shape[1]
    model_width = tokens.shape[2]
    full_len = seq_dev * lax.axis_size("ctx")
    positions = lax.axis_index("ctx") * seq_dev + jnp.arange(seq_dev, dtype=jnp.int32)
    live_mask = positions < lengths[0]
    live_rows = live_mask.astype(jnp.float32)[:, None]
    inputs = tokens[0].astype(jnp.float32)
    group = ("shard", "ctx")
    members = lax.axis_size(group)
    small = jnp.concatenate([attn_gain[None], ffn_gain[None], mix_weight.T], axis=0)
    small = lax.all_gather(small, group, axis=0)
    small = jnp.swapaxes(small, 0, 1).reshape(4, model_width)
    gain_one, gain_two, mix_full = small[0], small[1], small[2:].T
    qkv_full = lax.all_gather(
        jnp.swapaxes(qkv_weight, 0, 1), group, axis=1, tiled=True
    )
    proj_full = lax.all_gather(proj_weight, group, axis=1, tiled=True)
    up_full = lax.all_gather(up_weight, group, axis=0, tiled=True)
    down_full = lax.all_gather(down_weight, group, axis=1, tiled=True)
    gain_one = gain_one.astype(jnp.float32)
    gain_two = gain_two.astype(jnp.float32)
    normed, unit_one, inverse_one = norm_forward(inputs, gain_one)
    normed_low = normed.astype(jnp.bfloat16)
    ctx_size = lax.axis_size("ctx")
    projected = jnp.einsum(
        "cdf,td->cft", qkv_full, normed_low, preferred_element_type=jnp.float32
    ).astype(jnp.bfloat16)
    sent_qkv = jnp.swapaxes(projected.reshape(3, ctx_size, HD, seq_dev), 0, 1)
    qkv = lax.all_to_all(sent_qkv, "ctx", split_axis=0, concat_axis=0, tiled=True)
    heads_low, heads_wide, log_total = flash_forward(qkv)
    attended_low = lax.all_to_all(
        heads_low, "ctx", split_axis=0, concat_axis=0, tiled=True
    ).reshape(ctx_size * HD, seq_dev)
    branch_part = jnp.einsum(
        "ft,fd->td", attended_low, proj_full, preferred_element_type=jnp.float32
    )
    branch = lax.psum(branch_part.astype(jnp.bfloat16), "tp").astype(jnp.float32)
    middle = inputs + branch
    normed2, unit_two, inverse_two = norm_forward(middle, gain_two)
    normed2_low = normed2.astype(jnp.bfloat16)
    mixing = jax.nn.softmax(
        jnp.dot(normed2_low, mix_full, preferred_element_type=jnp.float32), axis=-1
    )
    upper_pre = jnp.dot(normed2_low, up_full, preferred_element_type=jnp.float32)
    hidden_low = gelu_tanh(upper_pre).astype(jnp.bfloat16)
    dense_part = jnp.dot(hidden_low, down_full, preferred_element_type=jnp.float32)
    experts_total = lax.axis_size(("shard", "ctx"))
    slot_cap = max(4, 3 * seq_dev // experts_total)
    chosen = routes[0, :, 0]
    onehot = (chosen[:, None] == jnp.arange(experts_total, dtype=jnp.int32)[None, :]).astype(
        jnp.int32
    )
    slot_pos = jnp.sum(jnp.cumsum(onehot, axis=0) * onehot, axis=1) - 1
    target = jnp.where(live_mask, chosen * slot_cap + slot_pos, experts_total * slot_cap)

    def pack_rows(token_rows):
        buffer = jnp.zeros((experts_total * slot_cap, model_width), token_rows.dtype)
        return (
            buffer.at[target]
            .set(token_rows, mode="drop")
            .reshape(experts_total, slot_cap, model_width)
        )

    send_order = (
        jnp.full((experts_total * slot_cap,), empty_mark, jnp.int32)
        .at[target]
        .set(priority[0], mode="drop")
    )
    recv_rows, recv_order = (
        lax.all_to_all(
            pack_rows(normed2_low), ("shard", "ctx"), split_axis=0, concat_axis=0, tiled=True
        ),
        lax.all_to_all(
            send_order.reshape(experts_total, slot_cap),
            ("shard", "ctx"),
            split_axis=0,
            concat_axis=0,
            tiled=True,
        ),
    )
    flat_order = recv_order.reshape(-1)
    ranking = jnp.argsort(flat_order)[:CAP]
    taken_mask = (flat_order[ranking] < empty_mark).astype(jnp.float32)[:, None]
    expert_in = recv_rows.reshape(-1, model_width)[ranking]
    own_up = expert_up[0]
    own_down = expert_down[0]
    expert_pre = jnp.dot(expert_in, own_up, preferred_element_type=jnp.float32)
    expert_hidden = gelu_tanh(expert_pre).astype(jnp.bfloat16)
    expert_part = jnp.dot(expert_hidden, own_down, preferred_element_type=jnp.float32) * taken_mask

    def unfold_rows(slot_rows):
        buffer = jnp.zeros((experts_total * slot_cap, model_width), jnp.float32)
        return buffer.at[ranking].set(slot_rows).reshape(experts_total, slot_cap, model_width)

    full_index = jnp.where(live_mask, chosen * slot_cap + slot_pos, 0)
    returned_rows = lax.all_to_all(
        unfold_rows(expert_part).astype(jnp.bfloat16),
        ("shard", "ctx"),
        split_axis=0,
        concat_axis=0,
        tiled=True,
    ).astype(jnp.float32)
    expert_tok = returned_rows.reshape(-1, model_width)[full_index] * live_rows
    mixed_part = mixing[:, 0:1] * dense_part + mixing[:, 1:2] * expert_tok
    mixed = lax.psum(mixed_part.astype(jnp.bfloat16), "tp").astype(jnp.float32)
    layer_out = ((middle + mixed) * live_rows).astype(jnp.bfloat16)[None]
    out_grad = cotangent[0].astype(jnp.float32) * live_rows
    dense_grad = (mixing[:, 0:1] * out_grad).astype(jnp.bfloat16)
    expert_grad = (mixing[:, 1:2] * out_grad).astype(jnp.bfloat16)
    dots_part = jnp.stack(
        [jnp.sum(out_grad * dense_part, axis=-1), jnp.sum(out_grad * expert_tok, axis=-1)], axis=-1
    )
    down_grad = jnp.einsum("tf,td->fd", hidden_low, dense_grad, preferred_element_type=jnp.float32)
    hidden_grad = jnp.einsum("td,fd->tf", dense_grad, down_full, preferred_element_type=jnp.float32)
    _, gelu_pull = jax.vjp(gelu_tanh, upper_pre)
    upper_grad = gelu_pull(hidden_grad)[0].astype(jnp.bfloat16)
    up_grad = jnp.einsum("td,tf->df", normed2_low, upper_grad, preferred_element_type=jnp.float32)
    normed2_part = jnp.einsum("tf,df->td", upper_grad, up_full, preferred_element_type=jnp.float32)
    recv_grad = lax.all_to_all(
        pack_rows(expert_grad), ("shard", "ctx"), split_axis=0, concat_axis=0, tiled=True
    )
    grad_in = recv_grad.reshape(-1, model_width)[ranking]
    own_down_grad = jnp.einsum(
        "cf,cd->fd", expert_hidden, grad_in, preferred_element_type=jnp.float32
    )
    ehidden_grad = jnp.einsum("cd,fd->cf", grad_in, own_down, preferred_element_type=jnp.float32)
    _, expert_pull = jax.vjp(gelu_tanh, expert_pre)
    epre_grad = expert_pull(ehidden_grad)[0].astype(jnp.bfloat16)
    own_up_grad = jnp.einsum("cd,cf->df", expert_in, epre_grad, preferred_element_type=jnp.float32)
    expert_in_grad = jnp.einsum("cf,df->cd", epre_grad, own_up, preferred_element_type=jnp.float32)
    sent_back = lax.all_to_all(
        unfold_rows(expert_in_grad).astype(jnp.bfloat16),
        ("shard", "ctx"),
        split_axis=0,
        concat_axis=0,
        tiled=True,
    ).astype(jnp.float32)
    expert_tok_grad = sent_back.reshape(-1, model_width)[full_index] * live_rows
    normed2_grad, branch_dots = (
        lax.psum((normed2_part + expert_tok_grad).astype(jnp.bfloat16), "tp").astype(jnp.float32),
        lax.psum(dots_part.astype(jnp.bfloat16), "tp").astype(jnp.float32),
    )
    logit_grad = mixing * (branch_dots - jnp.sum(mixing * branch_dots, axis=-1, keepdims=True))
    mix_grad = jnp.dot(
        normed2_low.astype(jnp.float32).T, logit_grad, precision=lax.Precision.HIGHEST
    )
    normed2_grad = normed2_grad + jnp.dot(
        logit_grad, mix_full.astype(jnp.float32).T, precision=lax.Precision.HIGHEST
    )
    middle_norm_grad, gain_two_grad = norm_backward(normed2_grad, gain_two, unit_two, inverse_two)
    middle_grad = out_grad + middle_norm_grad
    branch_grad = middle_grad.astype(jnp.bfloat16)
    proj_grad = jnp.einsum(
        "ft,td->fd", attended_low, branch_grad, preferred_element_type=jnp.float32
    )
    attended_grad = jnp.einsum(
        "fd,td->ft", proj_full, branch_grad, preferred_element_type=jnp.float32
    ).astype(jnp.bfloat16)
    heads_grad = lax.all_to_all(
        attended_grad.reshape(ctx_size, HD, seq_dev), "ctx", split_axis=0, concat_axis=0, tiled=True
    )
    sent_grad = flash_backward(qkv, heads_grad, heads_wide, log_total)
    qkv_grad = lax.all_to_all(sent_grad, "ctx", split_axis=0, concat_axis=0, tiled=True)
    qkv_grad = jnp.swapaxes(qkv_grad, 0, 1).reshape(3, ctx_size * HD, seq_dev)
    qkv_grad_full = jnp.einsum(
        "td,cft->cdf", normed_low, qkv_grad, preferred_element_type=jnp.float32
    )
    normed_part = jnp.einsum("cft,cdf->td", qkv_grad, qkv_full, preferred_element_type=jnp.float32)
    normed_grad = lax.psum(normed_part.astype(jnp.bfloat16), "tp").astype(jnp.float32)
    input_norm_grad, gain_one_grad = norm_backward(normed_grad, gain_one, unit_one, inverse_one)
    tokens_grad = (middle_grad + input_norm_grad).astype(jnp.bfloat16)[None]
    def shared(value, axis):
        return lax.psum_scatter(
            value.astype(jnp.bfloat16), group, scatter_dimension=axis, tiled=True
        ).astype(jnp.float32)

    small_grad = jnp.concatenate([gain_one_grad[None], gain_two_grad[None], mix_grad.T], axis=0)
    small_grad = jnp.swapaxes(small_grad.reshape(4, members, -1), 0, 1)
    small_grad = lax.psum_scatter(small_grad, group, scatter_dimension=0, tiled=True)[0]
    shares = (
        small_grad[0],
        jnp.swapaxes(shared(qkv_grad_full, 1), 0, 1),
        shared(proj_grad, 1),
        small_grad[1],
        small_grad[2:].T,
        shared(up_grad, 0),
        shared(down_grad, 1),
    )
    return (
        layer_out,
        tokens_grad,
        shares[0],
        shares[1],
        shares[2],
        shares[3],
        shares[4],
        shares[5],
        shares[6],
        own_up_grad[None],
        own_down_grad[None],
    )


def solution(mesh):
    placed = (
        P("shard", "ctx", None),
        P("shard"),
        P("shard", "ctx", None),
        P("shard", "ctx"),
        P(("shard", "ctx")),
        P(("shard", "ctx"), None, "tp"),
        P("tp", ("shard", "ctx")),
        P(("shard", "ctx")),
        P(("shard", "ctx"), None),
        P(("shard", "ctx"), "tp"),
        P("tp", ("shard", "ctx")),
        P(("shard", "ctx"), None, "tp"),
        P(("shard", "ctx"), "tp", None),
        P("shard", "ctx", None),
    )
    return jax.shard_map(
        local,
        mesh=mesh,
        in_specs=placed,
        out_specs=(
            P("shard", "ctx", None),
            P("shard", "ctx", None),
            P(("shard", "ctx")),
            P(("shard", "ctx"), None, "tp"),
            P("tp", ("shard", "ctx")),
            P(("shard", "ctx")),
            P(("shard", "ctx"), None),
            P(("shard", "ctx"), "tp"),
            P("tp", ("shard", "ctx")),
            P(("shard", "ctx"), None, "tp"),
            P(("shard", "ctx"), "tp", None),
        ),
        check_vma=False,
    )
```

```python
import jax
import jax.numpy as jnp
from jax import lax
from jax.experimental import pallas as pl
from jax.experimental.pallas import tpu as pltpu
from jax.sharding import PartitionSpec as P

HD = 64
CAP = 1152
TILE = 512


empty_mark = 1 << 30
norm_eps = 1e-05
masked_score = -1e30


def gelu_tanh(values):
    return jax.nn.gelu(values, approximate=True)


def norm_forward(values, gain_vec):
    average = jnp.mean(values, axis=-1, keepdims=True)
    centred = values - average
    spread = jnp.mean(centred * centred, axis=-1, keepdims=True)
    inverse = lax.rsqrt(spread + norm_eps)
    unit_rows = centred * inverse
    return (unit_rows * gain_vec, unit_rows, inverse)


def norm_backward(upstream, gain_vec, unit_rows, inverse):
    shaped = upstream * gain_vec
    first_term = jnp.mean(shaped, axis=-1, keepdims=True)
    second_term = jnp.mean(shaped * unit_rows, axis=-1, keepdims=True)
    return (
        inverse * (shaped - first_term - unit_rows * second_term),
        jnp.sum(upstream * unit_rows, axis=0),
    )

NT = (((1,), (1,)), ((), ()))


def tile_of(index, chunk):
    per = chunk // TILE
    return index // per, pl.ds(pl.multiple_of((index % per) * TILE, TILE), TILE)


def rows_of(index):
    return pl.ds(pl.multiple_of(index * TILE, TILE), TILE)


def causal():
    key_at = lax.broadcasted_iota(jnp.int32, (TILE, TILE), 0)
    query_at = lax.broadcasted_iota(jnp.int32, (TILE, TILE), 1)
    return key_at <= query_at


def flash_forward_body(qkv_ref, out_ref, wide_ref, lse_ref, key_rows):
    chunks, _, _, chunk = qkv_ref.shape
    tiles = chunks * chunk // TILE
    for c in range(chunks):
        key_rows[pl.ds(c * chunk, chunk), :] = qkv_ref[c, 1].T

    @pl.loop(0, tiles)
    def _(i):
        c, at = tile_of(i, chunk)
        query = qkv_ref[c, 0, :, at] * (HD ** (-0.5))

        def step(j, state, mask):
            top, total, acc = state
            kc, kat = tile_of(j, chunk)
            scores = jnp.dot(key_rows[rows_of(j), :], query, preferred_element_type=jnp.float32)
            if mask:
                scores = jnp.where(causal(), scores, masked_score)
            new_top = jnp.maximum(top, jnp.max(scores, axis=0, keepdims=True))
            shrink = jnp.exp(top - new_top)
            weights = jnp.exp(scores - new_top)
            total = total * shrink + jnp.sum(weights, axis=0, keepdims=True)
            acc = acc * shrink + jnp.dot(
                qkv_ref[kc, 2, :, kat],
                weights.astype(jnp.bfloat16),
                preferred_element_type=jnp.float32,
            )
            return new_top, total, acc

        state = (
            jnp.full((1, TILE), masked_score, jnp.float32),
            jnp.zeros((1, TILE), jnp.float32),
            jnp.zeros((HD, TILE), jnp.float32),
        )
        state = step(i, state, True)
        top, total, acc = lax.fori_loop(0, i, lambda j, s: step(j, s, False), state)
        result = acc / total
        wide_ref[c, :, at] = result
        out_ref[c, :, at] = result.astype(jnp.bfloat16)
        lse_ref[c, :, at] = top + jnp.log(total)


def flash_forward(qkv):
    chunks, _, width, chunk = qkv.shape
    return pl.pallas_call(
        flash_forward_body,
        name="flash_forward",
        out_shape=(
            jax.ShapeDtypeStruct((chunks, width, chunk), jnp.bfloat16),
            jax.ShapeDtypeStruct((chunks, width, chunk), jnp.float32),
            jax.ShapeDtypeStruct((chunks, 1, chunk), jnp.float32),
        ),
        scratch_shapes=[pltpu.VMEM((chunks * chunk, width), jnp.bfloat16)],
        cost_estimate=pl.CostEstimate(
            flops=2 * (chunks * chunk) ** 2 * width * 4, bytes_accessed=5 << 20, transcendentals=0
        ),
        compiler_params=pltpu.CompilerParams(vmem_limit_bytes=40 << 20),
    )(qkv)


def flash_backward_body(
    qkv_ref, grad_ref, wide_ref, lse_ref, out_ref,
    query_cols, query_rows, key_rows, value_rows, grad_rows, delta, query_grad,
):
    chunks, _, _, chunk = qkv_ref.shape
    tiles = chunks * chunk // TILE
    scale = HD ** (-0.5)
    for c in range(chunks):
        at = pl.ds(c * chunk, chunk)
        scaled = qkv_ref[c, 0] * scale
        query_cols[c] = scaled
        query_rows[at, :] = scaled.T
        key_rows[at, :] = qkv_ref[c, 1].T
        value_rows[at, :] = qkv_ref[c, 2].T
        grad_rows[at, :] = grad_ref[c].T
        delta[c] = jnp.sum(
            grad_ref[c].astype(jnp.float32) * wide_ref[c], axis=0, keepdims=True
        )
        query_grad[c] = jnp.zeros((HD, chunk), jnp.float32)

    @pl.loop(0, tiles)
    def _(j):
        kc, kat = tile_of(j, chunk)
        key_tile = key_rows[rows_of(j), :]
        value_tile = value_rows[rows_of(j), :]
        key_cols = qkv_ref[kc, 1, :, kat]

        def step(i, state, mask):
            key_grad, value_grad = state
            c, at = tile_of(i, chunk)
            scores = jnp.dot(key_tile, query_cols[c, :, at], preferred_element_type=jnp.float32)
            probs = jnp.exp(scores - lse_ref[c, :, at])
            if mask:
                probs = jnp.where(causal(), probs, 0.0)
            prob_grad = jnp.dot(value_tile, grad_ref[c, :, at], preferred_element_type=jnp.float32)
            score_grad = (probs * (prob_grad - delta[c, :, at])).astype(jnp.bfloat16)
            value_grad += jnp.dot(
                probs.astype(jnp.bfloat16), grad_rows[rows_of(i), :],
                preferred_element_type=jnp.float32,
            )
            key_grad += jnp.dot(
                score_grad, query_rows[rows_of(i), :], preferred_element_type=jnp.float32
            )
            query_grad[c, :, at] += jnp.dot(
                key_cols, score_grad, preferred_element_type=jnp.float32
            )
            return key_grad, value_grad

        state = (jnp.zeros((TILE, HD), jnp.float32), jnp.zeros((TILE, HD), jnp.float32))
        state = step(j, state, True)
        key_grad, value_grad = lax.fori_loop(
            j + 1, tiles, lambda i, s: step(i, s, False), state
        )
        out_ref[kc, 1, :, kat] = key_grad.T.astype(jnp.bfloat16)
        out_ref[kc, 2, :, kat] = value_grad.T.astype(jnp.bfloat16)

    for c in range(chunks):
        out_ref[c, 0] = (query_grad[c] * scale).astype(jnp.bfloat16)


def flash_backward(qkv, grad, wide, lse):
    chunks, _, width, chunk = qkv.shape
    full = chunks * chunk
    return pl.pallas_call(
        flash_backward_body,
        name="flash_backward",
        out_shape=jax.ShapeDtypeStruct((chunks, 3, width, chunk), jnp.bfloat16),
        scratch_shapes=[
            pltpu.VMEM((chunks, width, chunk), jnp.bfloat16),
            pltpu.VMEM((full, width), jnp.bfloat16),
            pltpu.VMEM((full, width), jnp.bfloat16),
            pltpu.VMEM((full, width), jnp.bfloat16),
            pltpu.VMEM((full, width), jnp.bfloat16),
            pltpu.VMEM((chunks, 1, chunk), jnp.float32),
            pltpu.VMEM((chunks, width, chunk), jnp.float32),
        ],
        cost_estimate=pl.CostEstimate(
            flops=2 * full ** 2 * width * 10, bytes_accessed=8 << 20, transcendentals=0
        ),
        compiler_params=pltpu.CompilerParams(vmem_limit_bytes=48 << 20),
    )(qkv, grad, wide, lse)


def local(
    tokens,
    lengths,
    routes,
    priority,
    attn_gain,
    qkv_weight,
    proj_weight,
    ffn_gain,
    mix_weight,
    up_weight,
    down_weight,
    expert_up,
    expert_down,
    cotangent,
):
    seq_dev = tokens.shape[1]
    model_width = tokens.shape[2]
    full_len = seq_dev * lax.axis_size("ctx")
    positions = lax.axis_index("ctx") * seq_dev + jnp.arange(seq_dev, dtype=jnp.int32)
    live_mask = positions < lengths[0]
    live_rows = live_mask.astype(jnp.float32)[:, None]
    inputs = tokens[0].astype(jnp.float32)
    group = ("shard", "ctx")
    members = lax.axis_size(group)
    tokens_total = members * seq_dev
    code = jnp.where(
        live_mask, routes[0, :, 0] * tokens_total + priority[0], members * tokens_total
    )
    small = [attn_gain[None], ffn_gain[None], mix_weight.T]
    small = jnp.concatenate(small, axis=0).astype(jnp.float32)
    small_width = small.shape[1]
    small = jnp.concatenate([small.reshape(-1), code.astype(jnp.float32)])
    small = lax.all_gather(small, group, axis=0)
    code_all = small[:, 4 * small_width :].reshape(-1).astype(jnp.int32)
    small = jnp.swapaxes(small[:, : 4 * small_width].reshape(members, 4, small_width), 0, 1)
    small = small.reshape(4, model_width)
    gain_one, gain_two, mix_full = small[0], small[1], small[2:].T.astype(jnp.bfloat16)
    own_code = code_all - lax.axis_index(group) * tokens_total
    mine = (own_code >= 0) & (own_code < tokens_total)
    sorted_code, ranking = lax.sort(
        (
            jnp.where(mine, own_code, empty_mark),
            lax.iota(jnp.int32, tokens_total),
        ),
        num_keys=1,
    )
    ranking = ranking[:CAP]
    taken = sorted_code[:CAP] < empty_mark
    taken_mask = taken.astype(jnp.float32)[:, None]
    place = jnp.where(taken, ranking, tokens_total)
    part_width = model_width // lax.axis_size("tp")

    def columns(value):
        return lax.dynamic_slice_in_dim(
            value, lax.axis_index("tp") * part_width, part_width, axis=1
        )

    def rows_for_expert(value):
        everyone = lax.all_gather(columns(value), group, axis=0, tiled=True)
        return lax.all_gather(everyone[ranking], "tp", axis=1, tiled=True)

    grad_rows = rows_for_expert(cotangent[0])
    qkv_full = lax.all_gather(
        jnp.swapaxes(qkv_weight, 0, 1), group, axis=1, tiled=True
    )
    proj_full = lax.all_gather(proj_weight, group, axis=1, tiled=True)
    up_full = lax.all_gather(up_weight, group, axis=0, tiled=True)
    down_full = lax.all_gather(down_weight, group, axis=1, tiled=True)
    gain_one = gain_one.astype(jnp.float32)
    gain_two = gain_two.astype(jnp.float32)
    normed, unit_one, inverse_one = norm_forward(inputs, gain_one)
    normed_low = normed.astype(jnp.bfloat16)
    ctx_size = lax.axis_size("ctx")
    projected = jnp.einsum(
        "cdf,td->cft", qkv_full, normed_low, preferred_element_type=jnp.float32
    ).astype(jnp.bfloat16)
    sent_qkv = jnp.swapaxes(projected.reshape(3, ctx_size, HD, seq_dev), 0, 1)
    qkv = lax.all_to_all(sent_qkv, "ctx", split_axis=0, concat_axis=0, tiled=True)
    heads_low, heads_wide, log_total = flash_forward(qkv)
    attended_low = lax.all_to_all(
        heads_low, "ctx", split_axis=0, concat_axis=0, tiled=True
    ).reshape(ctx_size * HD, seq_dev)
    branch_part = jnp.einsum(
        "ft,fd->td", attended_low, proj_full, preferred_element_type=jnp.float32
    )
    branch = lax.psum(branch_part.astype(jnp.bfloat16), "tp").astype(jnp.float32)
    middle = inputs + branch
    normed2, unit_two, inverse_two = norm_forward(middle, gain_two)
    normed2_low = normed2.astype(jnp.bfloat16)
    mixing = jax.nn.softmax(
        jnp.dot(normed2_low, mix_full, preferred_element_type=jnp.float32), axis=-1
    )
    upper_pre = jnp.dot(normed2_low, up_full, preferred_element_type=jnp.float32)
    hidden_low = gelu_tanh(upper_pre).astype(jnp.bfloat16)
    dense_part = jnp.dot(hidden_low, down_full, preferred_element_type=jnp.float32)
    own_up = expert_up[0]
    own_down = expert_down[0]
    expert_in = rows_for_expert(normed2_low)
    expert_mixing = jax.nn.softmax(
        jnp.dot(expert_in, mix_full, preferred_element_type=jnp.float32), axis=-1
    )
    grad_in = (expert_mixing[:, 1:2] * grad_rows.astype(jnp.float32) * taken_mask).astype(
        jnp.bfloat16
    )
    expert_pre = jnp.dot(expert_in, own_up, preferred_element_type=jnp.float32)
    expert_hidden = gelu_tanh(expert_pre).astype(jnp.bfloat16)
    expert_part = jnp.dot(expert_hidden, own_down, preferred_element_type=jnp.float32)

    def summed_columns(value):
        return lax.psum_scatter(
            value.astype(jnp.bfloat16), "tp", scatter_dimension=1, tiled=True
        )

    out_grad = cotangent[0].astype(jnp.float32) * live_rows
    dense_grad = (mixing[:, 0:1] * out_grad).astype(jnp.bfloat16)
    dense_cols = summed_columns(dense_part).astype(jnp.float32)
    expert_cols = summed_columns(expert_part)
    down_grad = jnp.einsum("tf,td->fd", hidden_low, dense_grad, preferred_element_type=jnp.float32)
    hidden_grad = jnp.einsum("td,fd->tf", dense_grad, down_full, preferred_element_type=jnp.float32)
    _, gelu_pull = jax.vjp(gelu_tanh, upper_pre)
    upper_grad = gelu_pull(hidden_grad)[0].astype(jnp.bfloat16)
    up_grad = jnp.einsum("td,tf->df", normed2_low, upper_grad, preferred_element_type=jnp.float32)
    normed2_part = jnp.einsum("tf,df->td", upper_grad, up_full, preferred_element_type=jnp.float32)
    own_down_grad = jnp.einsum(
        "cf,cd->fd", expert_hidden, grad_in, preferred_element_type=jnp.float32
    )
    ehidden_grad = jnp.einsum("cd,fd->cf", grad_in, own_down, preferred_element_type=jnp.float32)
    _, expert_pull = jax.vjp(gelu_tanh, expert_pre)
    epre_grad = expert_pull(ehidden_grad)[0].astype(jnp.bfloat16)
    own_up_grad = jnp.einsum("cd,cf->df", expert_in, epre_grad, preferred_element_type=jnp.float32)
    expert_in_grad = jnp.einsum("cf,df->cd", epre_grad, own_up, preferred_element_type=jnp.float32)
    grad_cols = summed_columns(expert_in_grad)
    normed2_cols = summed_columns(normed2_part).astype(jnp.float32)
    placed = (
        jnp.zeros((tokens_total, 2 * part_width), jnp.bfloat16)
        .at[place]
        .set(jnp.concatenate([expert_cols, grad_cols], axis=1), mode="drop", unique_indices=True)
    )
    returned = lax.psum_scatter(placed, group, scatter_dimension=0, tiled=True).astype(jnp.float32)
    expert_tok = returned[:, :part_width]
    mixed = mixing[:, 0:1] * dense_cols + mixing[:, 1:2] * expert_tok
    out_cols = ((columns(middle) + mixed) * live_rows).astype(jnp.bfloat16)
    layer_out = lax.all_gather(out_cols, "tp", axis=1, tiled=True)[None]
    grad_part = columns(out_grad)
    dots_part = jnp.stack(
        [jnp.sum(grad_part * dense_cols, axis=-1), jnp.sum(grad_part * expert_tok, axis=-1)]
    ).reshape(-1, part_width)
    normed2_cols = jnp.concatenate([normed2_cols + returned[:, part_width:], dots_part], axis=0)
    gathered = lax.all_gather(normed2_cols.astype(jnp.bfloat16), "tp", axis=0)
    gathered = gathered.astype(jnp.float32)
    normed2_grad = jnp.swapaxes(gathered[:, :seq_dev], 0, 1).reshape(seq_dev, model_width)
    branch_dots = jnp.sum(gathered[:, seq_dev:], axis=0).reshape(2, seq_dev).T
    logit_grad = mixing * (branch_dots - jnp.sum(mixing * branch_dots, axis=-1, keepdims=True))
    mix_grad = jnp.dot(
        normed2_low.astype(jnp.float32).T, logit_grad, precision=lax.Precision.HIGHEST
    )
    normed2_grad = normed2_grad + jnp.dot(
        logit_grad, mix_full.astype(jnp.float32).T, precision=lax.Precision.HIGHEST
    )
    middle_norm_grad, gain_two_grad = norm_backward(normed2_grad, gain_two, unit_two, inverse_two)
    middle_grad = out_grad + middle_norm_grad
    branch_grad = middle_grad.astype(jnp.bfloat16)
    proj_grad = jnp.einsum(
        "ft,td->fd", attended_low, branch_grad, preferred_element_type=jnp.float32
    )
    attended_grad = jnp.einsum(
        "fd,td->ft", proj_full, branch_grad, preferred_element_type=jnp.float32
    ).astype(jnp.bfloat16)
    heads_grad = lax.all_to_all(
        attended_grad.reshape(ctx_size, HD, seq_dev), "ctx", split_axis=0, concat_axis=0, tiled=True
    )
    sent_grad = flash_backward(qkv, heads_grad, heads_wide, log_total)
    qkv_grad = lax.all_to_all(sent_grad, "ctx", split_axis=0, concat_axis=0, tiled=True)
    qkv_grad = jnp.swapaxes(qkv_grad, 0, 1).reshape(3, ctx_size * HD, seq_dev)
    qkv_grad_full = jnp.einsum(
        "td,cft->cdf", normed_low, qkv_grad, preferred_element_type=jnp.float32
    )
    normed_part = jnp.einsum("cft,cdf->td", qkv_grad, qkv_full, preferred_element_type=jnp.float32)
    normed_grad = lax.psum(normed_part.astype(jnp.bfloat16), "tp").astype(jnp.float32)
    input_norm_grad, gain_one_grad = norm_backward(normed_grad, gain_one, unit_one, inverse_one)
    tokens_grad = (middle_grad + input_norm_grad).astype(jnp.bfloat16)[None]
    def shared(value, axis):
        return lax.psum_scatter(
            value.astype(jnp.bfloat16), group, scatter_dimension=axis, tiled=True
        ).astype(jnp.float32)

    small_grad = jnp.concatenate([gain_one_grad[None], gain_two_grad[None], mix_grad.T], axis=0)
    small_grad = jnp.swapaxes(small_grad.reshape(4, members, -1), 0, 1)
    small_grad = lax.psum_scatter(small_grad, group, scatter_dimension=0, tiled=True)[0]
    shares = (
        small_grad[0],
        jnp.swapaxes(shared(qkv_grad_full, 1), 0, 1),
        shared(proj_grad, 1),
        small_grad[1],
        small_grad[2:].T,
        shared(up_grad, 0),
        shared(down_grad, 1),
    )
    return (
        layer_out,
        tokens_grad,
        shares[0],
        shares[1],
        shares[2],
        shares[3],
        shares[4],
        shares[5],
        shares[6],
        own_up_grad[None],
        own_down_grad[None],
    )


def solution(mesh):
    placed = (
        P("shard", "ctx", None),
        P("shard"),
        P("shard", "ctx", None),
        P("shard", "ctx"),
        P(("shard", "ctx")),
        P(("shard", "ctx"), None, "tp"),
        P("tp", ("shard", "ctx")),
        P(("shard", "ctx")),
        P(("shard", "ctx"), None),
        P(("shard", "ctx"), "tp"),
        P("tp", ("shard", "ctx")),
        P(("shard", "ctx"), None, "tp"),
        P(("shard", "ctx"), "tp", None),
        P("shard", "ctx", None),
    )
    return jax.shard_map(
        local,
        mesh=mesh,
        in_specs=placed,
        out_specs=(
            P("shard", "ctx", None),
            P("shard", "ctx", None),
            P(("shard", "ctx")),
            P(("shard", "ctx"), None, "tp"),
            P("tp", ("shard", "ctx")),
            P(("shard", "ctx")),
            P(("shard", "ctx"), None),
            P(("shard", "ctx"), "tp"),
            P("tp", ("shard", "ctx")),
            P(("shard", "ctx"), None, "tp"),
            P(("shard", "ctx"), "tp", None),
        ),
        check_vma=False,
    )
```

```python
import jax
import jax.numpy as jnp
from jax import lax
from jax.experimental import pallas as pl
from jax.experimental.pallas import tpu as pltpu
from jax.sharding import PartitionSpec as P

HD = 64
CAP = 1152
TILE = 512


empty_mark = 1 << 30
norm_eps = 1e-05
masked_score = -1e30


def gelu_tanh(values):
    return jax.nn.gelu(values, approximate=True)


def norm_forward(values, gain_vec):
    average = jnp.mean(values, axis=-1, keepdims=True)
    centred = values - average
    spread = jnp.mean(centred * centred, axis=-1, keepdims=True)
    inverse = lax.rsqrt(spread + norm_eps)
    unit_rows = centred * inverse
    return (unit_rows * gain_vec, unit_rows, inverse)


def norm_backward(upstream, gain_vec, unit_rows, inverse):
    shaped = upstream * gain_vec
    first_term = jnp.mean(shaped, axis=-1, keepdims=True)
    second_term = jnp.mean(shaped * unit_rows, axis=-1, keepdims=True)
    return (
        inverse * (shaped - first_term - unit_rows * second_term),
        jnp.sum(upstream * unit_rows, axis=0),
    )

NT = (((1,), (1,)), ((), ()))


def tile_of(index, chunk):
    per = chunk // TILE
    return index // per, pl.ds(pl.multiple_of((index % per) * TILE, TILE), TILE)


def rows_of(index):
    return pl.ds(pl.multiple_of(index * TILE, TILE), TILE)


def causal():
    key_at = lax.broadcasted_iota(jnp.int32, (TILE, TILE), 0)
    query_at = lax.broadcasted_iota(jnp.int32, (TILE, TILE), 1)
    return key_at <= query_at


def flash_forward_body(qkv_ref, out_ref, wide_ref, lse_ref, key_rows):
    chunks, _, _, chunk = qkv_ref.shape
    tiles = chunks * chunk // TILE
    for c in range(chunks):
        key_rows[pl.ds(c * chunk, chunk), :] = qkv_ref[c, 1].T

    @pl.loop(0, tiles)
    def _(i):
        c, at = tile_of(i, chunk)
        query = qkv_ref[c, 0, :, at] * (HD ** (-0.5))

        def step(j, state, mask):
            top, total, acc = state
            kc, kat = tile_of(j, chunk)
            scores = jnp.dot(key_rows[rows_of(j), :], query, preferred_element_type=jnp.float32)
            if mask:
                scores = jnp.where(causal(), scores, masked_score)
            new_top = jnp.maximum(top, jnp.max(scores, axis=0, keepdims=True))
            shrink = jnp.exp(top - new_top)
            weights = jnp.exp(scores - new_top)
            total = total * shrink + jnp.sum(weights, axis=0, keepdims=True)
            acc = acc * shrink + jnp.dot(
                qkv_ref[kc, 2, :, kat],
                weights.astype(jnp.bfloat16),
                preferred_element_type=jnp.float32,
            )
            return new_top, total, acc

        state = (
            jnp.full((1, TILE), masked_score, jnp.float32),
            jnp.zeros((1, TILE), jnp.float32),
            jnp.zeros((HD, TILE), jnp.float32),
        )
        state = step(i, state, True)
        top, total, acc = lax.fori_loop(0, i, lambda j, s: step(j, s, False), state)
        result = acc / total
        wide_ref[c, :, at] = result
        out_ref[c, :, at] = result.astype(jnp.bfloat16)
        lse_ref[c, :, at] = top + jnp.log(total)


def flash_forward(qkv):
    chunks, _, width, chunk = qkv.shape
    return pl.pallas_call(
        flash_forward_body,
        name="flash_forward",
        out_shape=(
            jax.ShapeDtypeStruct((chunks, width, chunk), jnp.bfloat16),
            jax.ShapeDtypeStruct((chunks, width, chunk), jnp.float32),
            jax.ShapeDtypeStruct((chunks, 1, chunk), jnp.float32),
        ),
        scratch_shapes=[pltpu.VMEM((chunks * chunk, width), jnp.bfloat16)],
        cost_estimate=pl.CostEstimate(
            flops=24 * 10 ** 9, bytes_accessed=5 << 20, transcendentals=0
        ),
        compiler_params=pltpu.CompilerParams(vmem_limit_bytes=40 << 20),
    )(qkv)


def flash_backward_body(
    qkv_ref, grad_ref, wide_ref, lse_ref, out_ref,
    query_cols, query_rows, key_rows, value_rows, grad_rows, delta, query_grad,
):
    chunks, _, _, chunk = qkv_ref.shape
    tiles = chunks * chunk // TILE
    scale = HD ** (-0.5)
    for c in range(chunks):
        at = pl.ds(c * chunk, chunk)
        scaled = qkv_ref[c, 0] * scale
        query_cols[c] = scaled
        query_rows[at, :] = scaled.T
        key_rows[at, :] = qkv_ref[c, 1].T
        value_rows[at, :] = qkv_ref[c, 2].T
        grad_rows[at, :] = grad_ref[c].T
        delta[c] = jnp.sum(
            grad_ref[c].astype(jnp.float32) * wide_ref[c], axis=0, keepdims=True
        )
        query_grad[c] = jnp.zeros((HD, chunk), jnp.float32)

    @pl.loop(0, tiles)
    def _(j):
        kc, kat = tile_of(j, chunk)
        key_tile = key_rows[rows_of(j), :]
        value_tile = value_rows[rows_of(j), :]
        key_cols = qkv_ref[kc, 1, :, kat]

        def step(i, state, mask):
            key_grad, value_grad = state
            c, at = tile_of(i, chunk)
            scores = jnp.dot(key_tile, query_cols[c, :, at], preferred_element_type=jnp.float32)
            probs = jnp.exp(scores - lse_ref[c, :, at])
            if mask:
                probs = jnp.where(causal(), probs, 0.0)
            prob_grad = jnp.dot(value_tile, grad_ref[c, :, at], preferred_element_type=jnp.float32)
            score_grad = (probs * (prob_grad - delta[c, :, at])).astype(jnp.bfloat16)
            value_grad += jnp.dot(
                probs.astype(jnp.bfloat16), grad_rows[rows_of(i), :],
                preferred_element_type=jnp.float32,
            )
            key_grad += jnp.dot(
                score_grad, query_rows[rows_of(i), :], preferred_element_type=jnp.float32
            )
            query_grad[c, :, at] += jnp.dot(
                key_cols, score_grad, preferred_element_type=jnp.float32
            )
            return key_grad, value_grad

        state = (jnp.zeros((TILE, HD), jnp.float32), jnp.zeros((TILE, HD), jnp.float32))
        state = step(j, state, True)
        key_grad, value_grad = lax.fori_loop(
            j + 1, tiles, lambda i, s: step(i, s, False), state
        )
        out_ref[kc, 1, :, kat] = key_grad.T.astype(jnp.bfloat16)
        out_ref[kc, 2, :, kat] = value_grad.T.astype(jnp.bfloat16)

    for c in range(chunks):
        out_ref[c, 0] = (query_grad[c] * scale).astype(jnp.bfloat16)


def flash_backward(qkv, grad, wide, lse):
    chunks, _, width, chunk = qkv.shape
    full = chunks * chunk
    return pl.pallas_call(
        flash_backward_body,
        name="flash_backward",
        out_shape=jax.ShapeDtypeStruct((chunks, 3, width, chunk), jnp.bfloat16),
        scratch_shapes=[
            pltpu.VMEM((chunks, width, chunk), jnp.bfloat16),
            pltpu.VMEM((full, width), jnp.bfloat16),
            pltpu.VMEM((full, width), jnp.bfloat16),
            pltpu.VMEM((full, width), jnp.bfloat16),
            pltpu.VMEM((full, width), jnp.bfloat16),
            pltpu.VMEM((chunks, 1, chunk), jnp.float32),
            pltpu.VMEM((chunks, width, chunk), jnp.float32),
        ],
        cost_estimate=pl.CostEstimate(
            flops=32 * 10 ** 9, bytes_accessed=8 << 20, transcendentals=0
        ),
        compiler_params=pltpu.CompilerParams(vmem_limit_bytes=48 << 20),
    )(qkv, grad, wide, lse)


def local(
    tokens,
    lengths,
    routes,
    priority,
    attn_gain,
    qkv_weight,
    proj_weight,
    ffn_gain,
    mix_weight,
    up_weight,
    down_weight,
    expert_up,
    expert_down,
    cotangent,
):
    seq_dev = tokens.shape[1]
    model_width = tokens.shape[2]
    full_len = seq_dev * lax.axis_size("ctx")
    positions = lax.axis_index("ctx") * seq_dev + jnp.arange(seq_dev, dtype=jnp.int32)
    live_mask = positions < lengths[0]
    live_rows = live_mask.astype(jnp.float32)[:, None]
    inputs = tokens[0].astype(jnp.float32)
    group = ("shard", "ctx")
    members = lax.axis_size(group)
    tokens_total = members * seq_dev
    code = jnp.where(
        live_mask, routes[0, :, 0] * tokens_total + priority[0], members * tokens_total
    )
    small = [attn_gain[None], ffn_gain[None], mix_weight.T]
    small = jnp.concatenate(small, axis=0).astype(jnp.float32)
    small_width = small.shape[1]
    small = jnp.concatenate([small.reshape(-1), code.astype(jnp.float32)])
    small = lax.all_gather(small, group, axis=0)
    code_all = small[:, 4 * small_width :].reshape(-1).astype(jnp.int32)
    small = jnp.swapaxes(small[:, : 4 * small_width].reshape(members, 4, small_width), 0, 1)
    small = small.reshape(4, model_width)
    gain_one, gain_two, mix_full = small[0], small[1], small[2:].T.astype(jnp.bfloat16)
    own_code = code_all - lax.axis_index(group) * tokens_total
    mine = (own_code >= 0) & (own_code < tokens_total)
    sorted_code, ranking = lax.sort(
        (
            jnp.where(mine, own_code, empty_mark),
            lax.iota(jnp.int32, tokens_total),
        ),
        num_keys=1,
    )
    ranking = ranking[:CAP]
    taken = sorted_code[:CAP] < empty_mark
    taken_mask = taken.astype(jnp.float32)[:, None]
    place = jnp.where(taken, ranking, tokens_total)
    part_width = model_width // lax.axis_size("tp")

    def columns(value):
        return lax.dynamic_slice_in_dim(
            value, lax.axis_index("tp") * part_width, part_width, axis=1
        )

    def rows_for_expert(value):
        everyone = lax.all_gather(columns(value), group, axis=0, tiled=True)
        return lax.all_gather(everyone[ranking], "tp", axis=1, tiled=True)

    grad_rows = rows_for_expert(cotangent[0])
    qkv_full = lax.all_gather(
        jnp.swapaxes(qkv_weight, 0, 1), group, axis=1, tiled=True
    )
    proj_full = lax.all_gather(proj_weight, group, axis=1, tiled=True)
    up_full = lax.all_gather(up_weight, group, axis=0, tiled=True)
    down_full = lax.all_gather(down_weight, group, axis=1, tiled=True)
    gain_one = gain_one.astype(jnp.float32)
    gain_two = gain_two.astype(jnp.float32)
    normed, unit_one, inverse_one = norm_forward(inputs, gain_one)
    normed_low = normed.astype(jnp.bfloat16)
    ctx_size = lax.axis_size("ctx")
    projected = jnp.einsum(
        "cdf,td->cft", qkv_full, normed_low, preferred_element_type=jnp.float32
    ).astype(jnp.bfloat16)
    sent_qkv = jnp.swapaxes(projected.reshape(3, ctx_size, HD, seq_dev), 0, 1)
    qkv = lax.all_to_all(sent_qkv, "ctx", split_axis=0, concat_axis=0, tiled=True)
    heads_low, heads_wide, log_total = flash_forward(qkv)
    attended_low = lax.all_to_all(
        heads_low, "ctx", split_axis=0, concat_axis=0, tiled=True
    ).reshape(ctx_size * HD, seq_dev)
    branch_part = jnp.einsum(
        "ft,fd->td", attended_low, proj_full, preferred_element_type=jnp.float32
    )
    branch_low, up_full, down_full, grad_rows = lax.optimization_barrier(
        (branch_part.astype(jnp.bfloat16), up_full, down_full, grad_rows)
    )
    branch = lax.psum(branch_low, "tp").astype(jnp.float32)
    middle = inputs + branch
    normed2, unit_two, inverse_two = norm_forward(middle, gain_two)
    normed2_low = normed2.astype(jnp.bfloat16)
    mixing = jax.nn.softmax(
        jnp.dot(normed2_low, mix_full, preferred_element_type=jnp.float32), axis=-1
    )
    upper_pre = jnp.dot(normed2_low, up_full, preferred_element_type=jnp.float32)
    hidden_low = gelu_tanh(upper_pre).astype(jnp.bfloat16)
    dense_part = jnp.dot(hidden_low, down_full, preferred_element_type=jnp.float32)
    def summed_columns(value):
        return lax.psum_scatter(
            value.astype(jnp.bfloat16), "tp", scatter_dimension=1, tiled=True
        )

    out_grad = cotangent[0].astype(jnp.float32) * live_rows
    dense_grad = (mixing[:, 0:1] * out_grad).astype(jnp.bfloat16)
    down_grad = jnp.einsum("tf,td->fd", hidden_low, dense_grad, preferred_element_type=jnp.float32)
    hidden_grad = jnp.einsum("td,fd->tf", dense_grad, down_full, preferred_element_type=jnp.float32)
    _, gelu_pull = jax.vjp(gelu_tanh, upper_pre)
    upper_grad = gelu_pull(hidden_grad)[0].astype(jnp.bfloat16)
    up_grad = jnp.einsum("td,tf->df", normed2_low, upper_grad, preferred_element_type=jnp.float32)
    normed2_part = jnp.einsum("tf,df->td", upper_grad, up_full, preferred_element_type=jnp.float32)
    own_up = expert_up[0]
    own_down = expert_down[0]
    expert_in, dense_low, normed2_part = lax.optimization_barrier(
        (
            rows_for_expert(normed2_low),
            dense_part.astype(jnp.bfloat16),
            normed2_part.astype(jnp.bfloat16),
        )
    )
    dense_cols = summed_columns(dense_low)
    expert_mixing = jax.nn.softmax(
        jnp.dot(expert_in, mix_full, preferred_element_type=jnp.float32), axis=-1
    )
    grad_in = (expert_mixing[:, 1:2] * grad_rows.astype(jnp.float32) * taken_mask).astype(
        jnp.bfloat16
    )
    expert_pre = jnp.dot(expert_in, own_up, preferred_element_type=jnp.float32)
    expert_hidden = gelu_tanh(expert_pre).astype(jnp.bfloat16)
    expert_part = jnp.dot(expert_hidden, own_down, preferred_element_type=jnp.float32)

    expert_low, dense_cols = lax.optimization_barrier(
        (expert_part.astype(jnp.bfloat16), dense_cols)
    )
    dense_cols = dense_cols.astype(jnp.float32)
    expert_cols = summed_columns(expert_low)
    own_down_grad = jnp.einsum(
        "cf,cd->fd", expert_hidden, grad_in, preferred_element_type=jnp.float32
    )
    ehidden_grad = jnp.einsum("cd,fd->cf", grad_in, own_down, preferred_element_type=jnp.float32)
    _, expert_pull = jax.vjp(gelu_tanh, expert_pre)
    epre_grad = expert_pull(ehidden_grad)[0].astype(jnp.bfloat16)
    own_up_grad = jnp.einsum("cd,cf->df", expert_in, epre_grad, preferred_element_type=jnp.float32)
    expert_in_grad = jnp.einsum("cf,df->cd", epre_grad, own_up, preferred_element_type=jnp.float32)
    grad_cols = summed_columns(expert_in_grad)
    normed2_cols = summed_columns(normed2_part).astype(jnp.float32)
    placed = (
        jnp.zeros((tokens_total, 2 * part_width), jnp.bfloat16)
        .at[place]
        .set(jnp.concatenate([expert_cols, grad_cols], axis=1), mode="drop", unique_indices=True)
    )
    returned = lax.psum_scatter(placed, group, scatter_dimension=0, tiled=True).astype(jnp.float32)
    expert_tok = returned[:, :part_width]
    mixed = mixing[:, 0:1] * dense_cols + mixing[:, 1:2] * expert_tok
    out_cols = ((columns(middle) + mixed) * live_rows).astype(jnp.bfloat16)
    layer_out = lax.all_gather(out_cols, "tp", axis=1, tiled=True)[None]
    grad_part = columns(out_grad)
    dots_part = jnp.stack(
        [jnp.sum(grad_part * dense_cols, axis=-1), jnp.sum(grad_part * expert_tok, axis=-1)]
    ).reshape(-1, part_width)
    normed2_cols = jnp.concatenate([normed2_cols + returned[:, part_width:], dots_part], axis=0)
    gathered = lax.all_gather(normed2_cols.astype(jnp.bfloat16), "tp", axis=0)
    gathered = gathered.astype(jnp.float32)
    normed2_grad = jnp.swapaxes(gathered[:, :seq_dev], 0, 1).reshape(seq_dev, model_width)
    branch_dots = jnp.sum(gathered[:, seq_dev:], axis=0).reshape(2, seq_dev).T
    logit_grad = mixing * (branch_dots - jnp.sum(mixing * branch_dots, axis=-1, keepdims=True))
    mix_grad = jnp.dot(
        normed2_low.astype(jnp.float32).T, logit_grad, precision=lax.Precision.HIGHEST
    )
    normed2_grad = normed2_grad + jnp.dot(
        logit_grad, mix_full.astype(jnp.float32).T, precision=lax.Precision.HIGHEST
    )
    middle_norm_grad, gain_two_grad = norm_backward(normed2_grad, gain_two, unit_two, inverse_two)
    middle_grad = out_grad + middle_norm_grad
    branch_grad = middle_grad.astype(jnp.bfloat16)
    proj_grad = jnp.einsum(
        "ft,td->fd", attended_low, branch_grad, preferred_element_type=jnp.float32
    )
    attended_grad = jnp.einsum(
        "fd,td->ft", proj_full, branch_grad, preferred_element_type=jnp.float32
    ).astype(jnp.bfloat16)
    heads_grad = lax.all_to_all(
        attended_grad.reshape(ctx_size, HD, seq_dev), "ctx", split_axis=0, concat_axis=0, tiled=True
    )
    def shared(value, axis):
        return lax.psum_scatter(
            value.astype(jnp.bfloat16), group, scatter_dimension=axis, tiled=True
        ).astype(jnp.float32)

    sent_grad = flash_backward(qkv, heads_grad, heads_wide, log_total)
    sent_grad, layer_out, up_share, down_share, proj_share = lax.optimization_barrier(
        (sent_grad, layer_out, shared(up_grad, 0), shared(down_grad, 1), shared(proj_grad, 1))
    )
    qkv_grad = lax.all_to_all(sent_grad, "ctx", split_axis=0, concat_axis=0, tiled=True)
    qkv_grad = jnp.swapaxes(qkv_grad, 0, 1).reshape(3, ctx_size * HD, seq_dev)
    qkv_grad_full = jnp.einsum(
        "td,cft->cdf", normed_low, qkv_grad, preferred_element_type=jnp.float32
    )
    normed_part = jnp.einsum("cft,cdf->td", qkv_grad, qkv_full, preferred_element_type=jnp.float32)
    normed_grad = lax.psum(normed_part.astype(jnp.bfloat16), "tp").astype(jnp.float32)
    input_norm_grad, _ = norm_backward(normed_grad, gain_one, unit_one, inverse_one)
    tokens_grad = (middle_grad + input_norm_grad).astype(jnp.bfloat16)[None]
    gain_one_grad = jnp.sum(qkv_grad_full * qkv_full.astype(jnp.float32), axis=(0, 2)) / gain_one
    replicas = 1.0 / lax.axis_size("tp")
    small_grad = jnp.concatenate(
        [gain_one_grad[None], replicas * gain_two_grad[None], replicas * mix_grad.T], axis=0
    )
    small_grad = jnp.swapaxes(small_grad.reshape(4, members, -1), 0, 1)
    small_grad = lax.psum(small_grad, ("shard", "ctx", "tp"))[lax.axis_index(group)]
    shares = (
        small_grad[0],
        jnp.swapaxes(shared(qkv_grad_full, 1), 0, 1),
        proj_share,
        small_grad[1],
        small_grad[2:].T,
        up_share,
        down_share,
    )
    return (
        layer_out,
        tokens_grad,
        shares[0],
        shares[1],
        shares[2],
        shares[3],
        shares[4],
        shares[5],
        shares[6],
        own_up_grad[None],
        own_down_grad[None],
    )


def solution(mesh):
    placed = (
        P("shard", "ctx", None),
        P("shard"),
        P("shard", "ctx", None),
        P("shard", "ctx"),
        P(("shard", "ctx")),
        P(("shard", "ctx"), None, "tp"),
        P("tp", ("shard", "ctx")),
        P(("shard", "ctx")),
        P(("shard", "ctx"), None),
        P(("shard", "ctx"), "tp"),
        P("tp", ("shard", "ctx")),
        P(("shard", "ctx"), None, "tp"),
        P(("shard", "ctx"), "tp", None),
        P("shard", "ctx", None),
    )
    return jax.shard_map(
        local,
        mesh=mesh,
        in_specs=placed,
        out_specs=(
            P("shard", "ctx", None),
            P("shard", "ctx", None),
            P(("shard", "ctx")),
            P(("shard", "ctx"), None, "tp"),
            P("tp", ("shard", "ctx")),
            P(("shard", "ctx")),
            P(("shard", "ctx"), None),
            P(("shard", "ctx"), "tp"),
            P("tp", ("shard", "ctx")),
            P(("shard", "ctx"), None, "tp"),
            P(("shard", "ctx"), "tp", None),
        ),
        check_vma=False,
    )
```
